32 devices in a mesh: section: 2 (over x), tensor: 8 (over z, core), dp: 2 (over y).
Axes of the slice: x: 2, y: 2, z: 4, core: 2. Of those that a mesh axis runs over, the one named last changes fastest.
Arguments:
- dec_queries: bfloat16 [2, 4, 512, 8192], P('section', 'dp', None, 'tensor'), may hold values from -8 to 8
- enc_keys: bfloat16 [2, 4, 512, 8192], P('section', 'dp', None, 'tensor'), may hold values from -4 to 4
- enc_values: bfloat16 [2, 4, 512, 8192], P('section', 'dp', None, 'tensor'), may hold values from -4 to 4
- out_grad: bfloat16 [2, 4, 512, 8192], P('section', 'dp', None, 'tensor'), may hold values from -15 to 15
- key_weight: bfloat16 [2, 1024, 8192], P('section', None, 'tensor'), may hold values from -0.1875 to 0.1875
- value_weight: bfloat16 [2, 1024, 8192], P('section', None, 'tensor'), may hold values from -0.1875 to 0.1875
- enc_hidden: float32 [4, 512, 1024], P('dp', 'section', 'tensor'), may hold values from -2 to 2, as said below
- enc_gain: float32 [1024], P('tensor'), may hold values from 0.1 to 1.9
Outputs:
- enc_input_grad: float32 [4, 512, 1024], P('dp', 'section', 'tensor')
The draws below stay inside these ranges and needn't reach their ends.
Inputs may be any that keep to these rules, and one draw needn't show every extreme that they name: `enc_hidden`: every entry's magnitude is at least 0.25.
All inputs are finite; a program needn't handle non-finite values.
Results may differ from the reference program's by a relative error of at most 0.0041.
Values sent between devices are 32-bit elements; how exact they have to be, the bound alone decides.
A program may use at most 128 MiB of HBM per device.

```python
import jax
import jax.numpy as jnp
from jax import lax

D = 1024
DK = 128
DEC = 512
ENC = 512
HEADS = 64
INNER = 8192
SECTIONS = 2
SEQS = 4


def shared_rows(key):
    return jnp.clip(jax.random.normal(jax.random.fold_in(key, 12), (SECTIONS, SEQS, 1, INNER), jnp.float32), -4.0, 4.0)


def aligned_spot(key):
    return jax.random.randint(jax.random.fold_in(key, 13), (), 0, ENC).astype(jnp.int32)


def draw_enc_keys(key, part):
    base = jnp.clip(jax.random.normal(jax.random.fold_in(key, 11), (SECTIONS, SEQS, ENC, INNER), jnp.float32), -4.0, 4.0)
    zero = jnp.zeros((), jnp.int32)
    base = lax.dynamic_update_slice(base, shared_rows(key), (zero, zero, aligned_spot(key), zero))
    return base.astype(jnp.bfloat16)


def draw_dec_queries(key, part):
    base = 0.1 * jnp.clip(jax.random.normal(jax.random.fold_in(key, 22), (SECTIONS, SEQS, DEC, INNER), jnp.float32), -6.0, 6.0)
    return base.astype(jnp.bfloat16)


def draw_enc_hidden(key, part):
    shape = (SEQS, ENC, D)
    own_sign = jnp.where(jax.random.bernoulli(jax.random.fold_in(key, 31), 0.5, shape), 1.0, -1.0)
    magnitude = jax.random.uniform(jax.random.fold_in(key, 36), shape, jnp.float32, 0.25, 2.0)
    sign = own_sign
    return (sign * magnitude).astype(jnp.float32)


def levels(key, dims, cuts, smallest, high):
    factor_of, own = 1.0, jax.random.fold_in(key, 6)
    for position, parts in cuts:
        draws = jnp.exp(jax.random.uniform(jax.random.fold_in(own, position), (parts,), jnp.float32, smallest / len(cuts), high / len(cuts)))
        factor_of = factor_of * jnp.repeat(draws, dims[position] // parts).reshape([-1 if axis == position else 1 for axis in range(len(dims))])
    return factor_of


def normal_values(rng, extent, spread, most, shards=(), kind=jnp.bfloat16):
    values = jax.random.normal(rng, extent, jnp.float32) * spread
    if len(shards) > 0:
        values = levels(rng, extent, shards, -0.22, 0.18) * values
    return jnp.clip(values, min=-most, max=most).astype(kind)


def setup_inputs(seed: int = 0) -> dict:
    seeds = jax.random.split(jax.random.key(seed), 9)
    return {
        "dec_queries": draw_dec_queries(jax.random.fold_in(seeds[8], 71), 0),
        "enc_keys": draw_enc_keys(jax.random.fold_in(seeds[8], 71), 0),
        "enc_values": normal_values(seeds[2], (SECTIONS, SEQS, ENC, INNER), 1.0, 4.0, ((0, 2), (1, 2), (3, 8))),
        "out_grad": normal_values(seeds[3], (SECTIONS, SEQS, DEC, INNER), 3.0, 15.0, ((0, 2), (1, 2), (3, 8))),
        "key_weight": normal_values(seeds[4], (SECTIONS, D, INNER), D ** -0.5, 0.1875, ((0, 2), (2, 8))),
        "value_weight": normal_values(seeds[5], (SECTIONS, D, INNER), D ** -0.5, 0.1875, ((0, 2), (2, 8))),
        "enc_hidden": draw_enc_hidden(jax.random.fold_in(seeds[8], 71), 0),
        "enc_gain": jnp.clip(1.0 + 0.18 * jax.random.normal(seeds[7], (D,), jnp.float32), 0.1, 1.9),
    }


def attention_grads(query, keyset, valueset, gradset):
    query_heads = query.reshape(DEC, HEADS, DK).astype(jnp.float32)
    key_heads = keyset.reshape(ENC, HEADS, DK).astype(jnp.float32)
    value_heads = valueset.reshape(ENC, HEADS, DK).astype(jnp.float32)
    grad_heads = gradset.reshape(DEC, HEADS, DK).astype(jnp.float32)
    scores = jnp.einsum('qhd,khd->hqk', query_heads, key_heads)
    shifted = jnp.exp(scores - lax.optimization_barrier(jnp.max(scores, axis=-1, keepdims=True)))
    attn_probs = shifted / lax.optimization_barrier(jnp.sum(shifted, axis=-1, keepdims=True))
    probs_low = lax.optimization_barrier(attn_probs.astype(jnp.bfloat16)).astype(jnp.float32)
    attended = jnp.einsum('hqk,khd->qhd', probs_low, value_heads)
    row_dot = lax.optimization_barrier(jnp.sum(grad_heads * attended, axis=-1))
    value_grad = jnp.einsum('hqk,qhd->khd', probs_low, grad_heads).astype(jnp.bfloat16)
    prob_grad = jnp.einsum('qhd,khd->hqk', grad_heads, value_heads)
    score_grad = attn_probs * (prob_grad - jnp.transpose(row_dot)[:, :, None])
    score_low = lax.optimization_barrier(score_grad.astype(jnp.bfloat16)).astype(jnp.float32)
    key_grad = jnp.einsum('hqk,qhd->khd', score_low, query_heads).astype(jnp.bfloat16)
    return (key_grad.reshape(ENC, HEADS * DK), value_grad.reshape(ENC, HEADS * DK))

def reference(dec_queries, enc_keys, enc_values, out_grad, key_weight, value_weight, enc_hidden, enc_gain):

    def section_term(pieces):
        query, keyset, valueset, gradset, weight_k, weight_v = pieces

        def seq_term(inner):
            key_grad, value_grad = attention_grads(inner[0], inner[1], inner[2], inner[3])
            first = jnp.dot(key_grad, jnp.transpose(weight_k), preferred_element_type=jnp.float32)
            second = jnp.dot(value_grad, jnp.transpose(weight_v), preferred_element_type=jnp.float32)
            return first + second
        return lax.map(seq_term, (query, keyset, valueset, gradset))
    terms = lax.map(section_term, (dec_queries, enc_keys, enc_values, out_grad, key_weight, value_weight))
    enc_grad = lax.optimization_barrier(jnp.sum(terms, axis=0))
    scaled = enc_gain * enc_grad
    square_total = lax.optimization_barrier(jnp.sum(enc_hidden * enc_hidden, axis=-1))
    cross_total = lax.optimization_barrier(jnp.sum(scaled * enc_hidden, axis=-1))
    inverse = lax.rsqrt(square_total / D + 1e-06)
    return scaled * inverse[..., None] - enc_hidden * (cross_total * inverse * inverse * inverse / D)[..., None]
```

```python
import functools

import jax
import jax.numpy as jnp
from jax import lax
from jax.experimental import pallas as pl
from jax.experimental.pallas import tpu as pltpu
from jax.sharding import PartitionSpec as P

DK = 128
CORES = 2
EPSILON = 1e-06
MESH = pl.DeviceIdType.MESH
F32 = jnp.float32
BF16 = jnp.bfloat16
QUERY_BLOCK = 256
PIECES = 2


def dot_nt(a, b, precision=None):
    return lax.dot_general(
        a, b, (((1,), (1,)), ((), ())), precision=precision, preferred_element_type=F32
    )


def dot_nn(a, b):
    return lax.dot_general(a, b, (((1,), (0,)), ((), ())), preferred_element_type=F32)


def dot_tn(a, b, precision=None):
    return lax.dot_general(
        a, b, (((0,), (0,)), ((), ())), precision=precision, preferred_element_type=F32
    )


def body(
    sections, tensors, query_block,
    q_hbm, k_hbm, v_hbm, g_hbm, wk_hbm, wv_hbm, hidden_hbm, gain_hbm,
    out_ref,
    q_buf, k_buf, v_buf, g_buf, w_buf, hidden, gain, grads,
    scores_even, prob_grad_even, peak_even, scores_odd, prob_grad_odd, peak_odd,
    part, pair_in, section_in, line_out, line_in,
    square_out, square_in, cross_out, cross_in, inverse_wide, hidden_scaled,
    load_sem, weight_sem, small_sem,
    pair_send, pair_recv, section_send, section_recv, line_send, line_recv,
    square_send, square_recv, cross_send, cross_recv,
):
    seqs, heads, dec_len, _ = q_buf.shape
    enc_len = k_buf.shape[2]
    inner = heads * DK
    model_width = w_buf.shape[0]
    feats = out_ref.shape[2]
    rows = out_ref.shape[1]
    chips = tensors // CORES
    s_me = lax.axis_index("section")
    t_me = lax.axis_index("tensor")
    z_me = lax.div(t_me, CORES)
    c_me = lax.rem(t_me, CORES)
    partner = z_me * CORES + (CORES - 1 - c_me)
    pieces = PIECES
    piece_rows = rows // pieces

    def loads(b, h):
        cols = pl.ds(pl.multiple_of(h * DK, DK), DK)
        return [
            pltpu.make_async_copy(src.at[0, b, :, cols], dst.at[b, h], load_sem.at[i, b, h])
            for i, (src, dst) in enumerate(
                ((q_hbm, q_buf), (k_hbm, k_buf), (v_hbm, v_buf), (g_hbm, g_buf))
            )
        ]

    def start_loads(b):
        def step(h, carry):
            for copy in loads(b, h):
                copy.start()
            return carry

        lax.fori_loop(0, heads, step, 0)

    weight_copies = [
        pltpu.make_async_copy(src.at[0], w_buf.at[:, pl.ds(i * inner, inner)], weight_sem.at[i])
        for i, src in enumerate((wk_hbm, wv_hbm))
    ]
    small_copies = [
        pltpu.make_async_copy(hidden_hbm, hidden, small_sem.at[0]),
        pltpu.make_async_copy(gain_hbm, gain, small_sem.at[1]),
    ]

    start_loads(0)
    for copy in small_copies + weight_copies:
        copy.start()
    for b in range(1, seqs):
        start_loads(b)

    barrier = pltpu.get_barrier_semaphore()
    for i in range(1, tensors):
        pl.semaphore_signal(
            barrier, inc=1, device_id={"tensor": lax.rem(t_me + i, tensors)}, device_id_type=MESH
        )
    for i in range(1, sections):
        pl.semaphore_signal(
            barrier, inc=1, device_id={"section": lax.rem(s_me + i, sections)}, device_id_type=MESH
        )

    blocks = dec_len // query_block

    def wait_loads(i):
        for copy in loads(lax.div(i, heads), lax.rem(i, heads)):
            copy.wait()

    def score_step(i, bufs):
        scores_buf, prob_grad_buf, peak_buf = bufs
        b, h = lax.div(i, heads), lax.rem(i, heads)
        keys = k_buf[b, h]
        values = v_buf[b, h]
        for n in range(blocks):
            span = pl.ds(n * query_block, query_block)
            scores = dot_nt(keys, q_buf[b, h, span, :])
            scores_buf[n] = scores
            peak_buf[n] = jnp.max(scores, axis=0, keepdims=True)
            prob_grad_buf[n] = dot_nt(values, g_buf[b, h, span, :])

    def grad_step(i, bufs):
        scores_buf, prob_grad_buf, peak_buf = bufs
        b, h = lax.div(i, heads), lax.rem(i, heads)
        key_grad = None
        for n in range(blocks):
            span = pl.ds(n * query_block, query_block)
            shifted = jnp.exp(scores_buf[n] - peak_buf[n])
            scale = 1.0 / jnp.sum(shifted, axis=0, keepdims=True)
            probs_low = (shifted * scale).astype(BF16)
            row_dot = jnp.sum(probs_low.astype(F32) * prob_grad_buf[n], axis=0, keepdims=True)
            score_low = probs_low * (prob_grad_buf[n] - row_dot).astype(BF16)
            value_term = dot_nn(probs_low, g_buf[b, h, span, :])
            key_term = dot_nn(score_low, q_buf[b, h, span, :])
            if key_grad is None:
                key_grad, value_grad = key_term, value_term
            else:
                key_grad, value_grad = key_grad + key_term, value_grad + value_term
        grads[:, pl.ds(pl.multiple_of(h * DK, DK), DK)] = key_grad.astype(BF16)
        grads[:, pl.ds(pl.multiple_of(inner + h * DK, DK), DK)] = value_grad.astype(BF16)

    even = (scores_even, prob_grad_even, peak_even)
    odd = (scores_odd, prob_grad_odd, peak_odd)

    def head_pair(i):
        wait_loads(i + 1)
        score_step(i + 1, odd)
        grad_step(i, even)
        following = jnp.minimum(i + 2, seqs * heads - 1)

        @pl.when(i + 2 < seqs * heads)
        def _():
            wait_loads(i + 2)

        score_step(following, even)
        grad_step(i + 1, odd)

    def order(j):
        if chips & (chips - 1):
            return lax.rem(z_me + 1 + j, chips)
        chip, unit = 0, 1
        while unit < chips:
            bits = lax.div(z_me, unit) + lax.div(chips - 1 - j, unit)
            chip = chip + unit * lax.rem(bits, 2)
            unit *= 2
        return chip

    def section_of(i):
        return lax.rem(s_me + i, sections)

    def piece(r):
        return pl.ds(r * piece_rows, piece_rows)

    def pair_copy(b, i, j):
        return pltpu.make_async_remote_copy(
            src_ref=part.at[b, i, j, CORES - 1 - c_me], dst_ref=pair_in.at[b, i, j],
            send_sem=pair_send.at[b, i, j], recv_sem=pair_recv.at[b, i, j],
            device_id={"tensor": partner}, device_id_type=MESH,
        )

    def section_copy(b, i, j, r):
        return pltpu.make_async_remote_copy(
            src_ref=part.at[b, i, j, c_me, piece(r)], dst_ref=section_in.at[b, i - 1, j, piece(r)],
            send_sem=section_send.at[b, i - 1, j, r], recv_sem=section_recv.at[b, i - 1, j, r],
            device_id={"section": section_of(i)}, device_id_type=MESH,
        )

    def line_copy(b, j, r):
        return pltpu.make_async_remote_copy(
            src_ref=line_out.at[b, j, piece(r)], dst_ref=line_in.at[b, j, piece(r)],
            send_sem=line_send.at[b, j, r], recv_sem=line_recv.at[b, j, r],
            device_id={"tensor": order(j) * CORES + c_me}, device_id_type=MESH,
        )

    def stat_copies(src, dst, send, recv):
        return [
            pltpu.make_async_remote_copy(
                src_ref=src, dst_ref=dst.at[i - 1],
                send_sem=send.at[i - 1], recv_sem=recv.at[i - 1],
                device_id={"tensor": lax.rem(t_me + i, tensors)}, device_id_type=MESH,
            )
            for i in range(1, tensors)
        ]

    def square_copies():
        return stat_copies(square_out, square_in, square_send, square_recv)

    def cross_copies(b):
        return stat_copies(
            cross_out.at[b], cross_in.at[b], cross_send.at[b], cross_recv.at[b]
        )

    def lane_sums(x):
        total = dot_nt(jnp.ones((8, feats), F32), x, lax.Precision.HIGHEST)
        return total[0:1, :]

    def spread(row):
        return dot_tn(
            jnp.broadcast_to(row, (8, rows)), jnp.full((8, feats), 0.125, F32),
            lax.Precision.HIGHEST,
        )

    def loop(low, high, step):
        def run(i, carry):
            step(i)
            return carry

        lax.fori_loop(low, high, run, 0)

    def project(b, i, j):
        width = CORES * feats
        block = dot_nt(
            grads[pl.ds(pl.multiple_of(section_of(i) * rows, rows), rows), :],
            w_buf[pl.ds(pl.multiple_of(order(j) * width, width), width), :],
        )
        for half in range(CORES):
            part[b, i, j, half] = block[:, half * feats : (half + 1) * feats]
        pair_copy(b, i, j).start()

    def send_section(b, i, j):
        pair_copy(b, i, j).wait_recv()
        for r in range(pieces):
            part[b, i, j, c_me, piece(r)] += pair_in[b, i, j, piece(r)]
            section_copy(b, i, j, r).start()

    def project_all(b):
        for i in range(1, sections):
            project(b, i, 0)

            def step(j):
                project(b, i, j)
                send_section(b, i, j - 1)

            loop(1, chips, step)
            if i + 1 < sections:
                send_section(b, i, chips - 1)
        project(b, 0, 0)
        send_section(b, sections - 1, chips - 1)
        loop(1, chips, lambda j: project(b, 0, j))

    def gather_section(b, j):
        pair_copy(b, 0, j).wait_recv()
        for r in range(pieces):
            total = part[b, 0, j, c_me, piece(r)] + pair_in[b, 0, j, piece(r)]
            for i in range(1, sections):
                section_copy(b, i, j, r).wait_recv()
                total = total + section_in[b, i - 1, j, piece(r)]
            line_out[b, j, piece(r)] = total

            @pl.when(j < chips - 1)
            def _():
                line_copy(b, j, r).start()

    def finish_sum(b):
        for r in range(pieces):
            total = line_out[b, chips - 1, piece(r)]
            for j in range(chips - 1):
                line_copy(b, j, r).wait_recv()
                total = total + line_in[b, j, piece(r)]
            out_ref[b, piece(r)] = gain[...] * total
        cross_out[b] = lane_sums(out_ref[b] * hidden[b])
        for copy in cross_copies(b):
            copy.start()
        out_ref[b] = out_ref[b] * inverse_wide[b]

    def prepare_norm():
        for copy in square_copies():
            copy.wait_recv()
        for b in range(seqs):
            square = square_out[b]
            for i in range(tensors - 1):
                square = square + square_in[i, b]
            inverse = lax.rsqrt(square / model_width + EPSILON)
            inverse_wide[b] = spread(inverse)
            hidden_scaled[b] = hidden[b] * spread(inverse * inverse * inverse / model_width)

    def finish_norm(b):
        cross = cross_out[b]
        for i, copy in enumerate(cross_copies(b)):
            copy.wait_recv()
            cross = cross + cross_in[b, i]
        out_ref[b] = out_ref[b] - hidden_scaled[b] * spread(cross)

    steps = heads // 2
    wait_loads(0)
    score_step(0, even)
    for b in range(seqs):
        def heads_step(j):
            head_pair(b * heads + 2 * j)
            if b > 0:
                @pl.when((j > 0) & (j <= chips))
                def _():
                    gather_section(b - 1, j - 1)

        loop(0, steps, heads_step)
        if b == 0:
            for copy in small_copies:
                copy.wait()
            for copy in weight_copies:
                copy.wait()
            pl.semaphore_wait(barrier, tensors - 1 + sections - 1)
        project_all(b)
        if b == 0:
            for i in range(seqs):
                square_out[i] = lane_sums(hidden[i] * hidden[i])
            for copy in square_copies():
                copy.start()
        else:
            for j in range(min(steps - 1, chips), chips):
                gather_section(b - 1, j)
    prepare_norm()
    last = seqs - 1
    loop(0, chips // 2, lambda j: gather_section(last, j))
    for b in range(seqs - 1):
        finish_sum(b)
    loop(chips // 2, chips, lambda j: gather_section(last, j))
    finish_sum(last)
    for b in range(seqs):
        finish_norm(b)

    for copy in square_copies():
        copy.wait_send()
    for b in range(seqs):
        for copy in cross_copies(b):
            copy.wait_send()

        def drain(j):
            for i in range(sections):
                pair_copy(b, i, j).wait_send()
                for r in range(pieces if i else 0):
                    section_copy(b, i, j, r).wait_send()

        def drain_line(j):
            for r in range(pieces):
                line_copy(b, j, r).wait_send()

        loop(0, chips, drain)
        loop(0, chips - 1, drain_line)


def per_device(
    sections, tensors,
    dec_queries, enc_keys, enc_values, out_grad, key_weight, value_weight, enc_hidden, enc_gain,
):
    _, seqs, dec_len, inner = dec_queries.shape
    enc_len = enc_keys.shape[2]
    heads = inner // DK
    model_width = key_weight.shape[1]
    chips = tensors // CORES
    feats = model_width // tensors
    rows = enc_len // sections
    dma = pltpu.SemaphoreType.DMA
    query_block = min(QUERY_BLOCK, dec_len)
    blocks = dec_len // query_block
    unit = [
        pltpu.VMEM((blocks, enc_len, query_block), F32),
        pltpu.VMEM((blocks, enc_len, query_block), F32),
        pltpu.VMEM((blocks, 1, query_block), F32),
    ]
    call = pl.pallas_call(
        functools.partial(body, sections, tensors, query_block),
        out_shape=jax.ShapeDtypeStruct((seqs, rows, feats), F32),
        in_specs=[pl.BlockSpec(memory_space=pl.ANY)] * 8,
        out_specs=pl.BlockSpec(memory_space=pltpu.VMEM),
        scratch_shapes=[
            pltpu.VMEM((seqs, heads, dec_len, DK), BF16),
            pltpu.VMEM((seqs, heads, enc_len, DK), BF16),
            pltpu.VMEM((seqs, heads, enc_len, DK), BF16),
            pltpu.VMEM((seqs, heads, dec_len, DK), BF16),
            pltpu.VMEM((model_width, 2 * inner), BF16),
            pltpu.VMEM((seqs, rows, feats), F32),
            pltpu.VMEM((1, feats), F32),
            pltpu.VMEM((enc_len, 2 * inner), BF16),
            *unit, *unit,
            pltpu.VMEM((seqs, sections, chips, CORES, rows, feats), F32),
            pltpu.VMEM((seqs, sections, chips, rows, feats), F32),
            pltpu.VMEM((seqs, sections - 1, chips, rows, feats), F32),
            pltpu.VMEM((seqs, chips, rows, feats), F32),
            pltpu.VMEM((seqs, chips - 1, rows, feats), F32),
            pltpu.VMEM((seqs, 1, rows), F32),
            pltpu.VMEM((tensors - 1, seqs, 1, rows), F32),
            pltpu.VMEM((seqs, 1, rows), F32),
            pltpu.VMEM((seqs, tensors - 1, 1, rows), F32),
            pltpu.VMEM((seqs, rows, feats), F32),
            pltpu.VMEM((seqs, rows, feats), F32),
            dma((4, seqs, heads)),
            dma((2,)),
            dma((2,)),
            dma((seqs, sections, chips)),
            dma((seqs, sections, chips)),
            dma((seqs, sections - 1, chips, PIECES)),
            dma((seqs, sections - 1, chips, PIECES)),
            dma((seqs, chips - 1, PIECES)),
            dma((seqs, chips - 1, PIECES)),
            dma((tensors - 1,)),
            dma((tensors - 1,)),
            dma((seqs, tensors - 1)),
            dma((seqs, tensors - 1)),
        ],
        compiler_params=pltpu.CompilerParams(
            collective_id=0, has_side_effects=True, vmem_limit_bytes=60 * 1024 * 1024
        ),
    )
    return call(
        dec_queries, enc_keys, enc_values, out_grad, key_weight, value_weight,
        enc_hidden, enc_gain.reshape(1, feats),
    )


def solution(mesh):
    wide = P("section", "dp", None, "tensor")
    return jax.shard_map(
        functools.partial(per_device, mesh.shape["section"], mesh.shape["tensor"]),
        mesh=mesh,
        in_specs=(
            wide, wide, wide, wide,
            P("section", None, "tensor"),
            P("section", None, "tensor"),
            P("dp", "section", "tensor"),
            P("tensor"),
        ),
        out_specs=P("dp", "section", "tensor"),
        check_vma=False,
    )
```

```python
import functools

import jax
import jax.numpy as jnp
from jax import lax
from jax.experimental import pallas as pl
from jax.experimental.pallas import tpu as pltpu
from jax.sharding import PartitionSpec as P

DK = 128
CORES = 2
EPSILON = 1e-06
MESH = pl.DeviceIdType.MESH
F32 = jnp.float32
BF16 = jnp.bfloat16
QUERY_BLOCK = 256
PIECES = 4


def dot_nt(a, b, precision=None):
    return lax.dot_general(
        a, b, (((1,), (1,)), ((), ())), precision=precision, preferred_element_type=F32
    )


def dot_nn(a, b):
    return lax.dot_general(a, b, (((1,), (0,)), ((), ())), preferred_element_type=F32)


def dot_tn(a, b, precision=None):
    return lax.dot_general(
        a, b, (((0,), (0,)), ((), ())), precision=precision, preferred_element_type=F32
    )


def body(
    sections, tensors, query_block,
    q_hbm, k_hbm, v_hbm, g_hbm, wk_hbm, wv_hbm, hidden_hbm, gain_hbm,
    out_ref,
    qg_buf, kv_buf, w_buf, hidden, gain, grads,
    scores_even, prob_grad_even, peak_even, scores_odd, prob_grad_odd, peak_odd,
    part, pair_in, section_in, line_out, line_in,
    square_out, square_in, cross_out, cross_in, inverse_wide, hidden_scaled,
    load_sem, weight_sem, small_sem,
    pair_send, pair_recv, section_send, section_recv, line_send, line_recv,
    square_send, square_recv, cross_send, cross_recv,
):
    seqs, heads, _, dec_len, _ = qg_buf.shape
    enc_len = kv_buf.shape[3]
    inner = heads * DK
    model_width = w_buf.shape[0]
    feats = out_ref.shape[2]
    rows = out_ref.shape[1]
    chips = tensors // CORES
    s_me = lax.axis_index("section")
    t_me = lax.axis_index("tensor")
    z_me = lax.div(t_me, CORES)
    c_me = lax.rem(t_me, CORES)
    partner = z_me * CORES + (CORES - 1 - c_me)
    pieces = PIECES
    at_end = (z_me == 0) | (z_me == chips - 1)
    piece_rows = rows // pieces

    def loads(b, h):
        cols = pl.ds(pl.multiple_of(h * DK, DK), DK)
        return [
            pltpu.make_async_copy(src.at[0, b, :, cols], dst.at[b, h, n], load_sem.at[i, b, h])
            for i, (sources, dst) in enumerate((((q_hbm, g_hbm), qg_buf), ((k_hbm, v_hbm), kv_buf)))
            for n, src in enumerate(sources)
        ]

    def settle(ref, sem):
        pltpu.make_async_copy(ref, ref, sem).wait()

    def start_loads(b):
        def step(h, carry):
            for copy in loads(b, h):
                copy.start()
            return carry

        lax.fori_loop(0, heads, step, 0)

    weight_copies = [
        pltpu.make_async_copy(src.at[0], w_buf.at[:, pl.ds(i * inner, inner)], weight_sem)
        for i, src in enumerate((wk_hbm, wv_hbm))
    ]
    small_copies = [
        pltpu.make_async_copy(hidden_hbm, hidden, small_sem.at[0]),
        pltpu.make_async_copy(gain_hbm, gain, small_sem.at[1]),
    ]

    start_loads(0)
    for copy in small_copies + weight_copies:
        copy.start()
    for b in range(1, seqs):
        start_loads(b)

    barrier = pltpu.get_barrier_semaphore()
    for i in range(1, tensors):
        pl.semaphore_signal(
            barrier, inc=1, device_id={"tensor": lax.rem(t_me + i, tensors)}, device_id_type=MESH
        )
    for i in range(1, sections):
        pl.semaphore_signal(
            barrier, inc=1, device_id={"section": lax.rem(s_me + i, sections)}, device_id_type=MESH
        )

    blocks = dec_len // query_block

    def wait_loads(i):
        b, h = lax.div(i, heads), lax.rem(i, heads)
        settle(qg_buf.at[b, h], load_sem.at[0, b, h])
        settle(kv_buf.at[b, h], load_sem.at[1, b, h])

    def score_step(i, bufs):
        scores_buf, prob_grad_buf, peak_buf = bufs
        b, h = lax.div(i, heads), lax.rem(i, heads)
        keys = kv_buf[b, h, 0]
        values = kv_buf[b, h, 1]
        for n in range(blocks):
            span = pl.ds(n * query_block, query_block)
            scores = dot_nt(keys, qg_buf[b, h, 0, span, :])
            scores_buf[n] = scores
            peak_buf[n] = jnp.max(scores, axis=0, keepdims=True)
            prob_grad_buf[n] = dot_nt(values, qg_buf[b, h, 1, span, :])

    def grad_step(i, bufs):
        scores_buf, prob_grad_buf, peak_buf = bufs
        b, h = lax.div(i, heads), lax.rem(i, heads)
        key_grad = None
        for n in range(blocks):
            span = pl.ds(n * query_block, query_block)
            shifted = jnp.exp(scores_buf[n] - peak_buf[n])
            scale = 1.0 / jnp.sum(shifted, axis=0, keepdims=True)
            probs = shifted * scale
            probs_low = probs.astype(BF16)
            row_dot = jnp.sum(probs_low.astype(F32) * prob_grad_buf[n], axis=0, keepdims=True)
            score_low = (probs * (prob_grad_buf[n] - row_dot)).astype(BF16)
            value_term = dot_nn(probs_low, qg_buf[b, h, 1, span, :])
            key_term = dot_nn(score_low, qg_buf[b, h, 0, span, :])
            if key_grad is None:
                key_grad, value_grad = key_term, value_term
            else:
                key_grad, value_grad = key_grad + key_term, value_grad + value_term
        grads[:, pl.ds(pl.multiple_of(h * DK, DK), DK)] = key_grad.astype(BF16)
        grads[:, pl.ds(pl.multiple_of(inner + h * DK, DK), DK)] = value_grad.astype(BF16)

    even = (scores_even, prob_grad_even, peak_even)
    odd = (scores_odd, prob_grad_odd, peak_odd)

    def head_pair(i):
        wait_loads(i + 1)
        score_step(i + 1, odd)
        grad_step(i, even)
        following = jnp.minimum(i + 2, seqs * heads - 1)

        @pl.when(i + 2 < seqs * heads)
        def _():
            wait_loads(i + 2)

        score_step(following, even)
        grad_step(i + 1, odd)

    lower = z_me < chips // 2
    ahead = jnp.where(lower, chips - 1 - z_me, z_me)

    def order(j):
        rising = jnp.where(j < ahead, j, j - ahead)
        falling = chips - 1 - rising
        chip = jnp.where(lower == (j < ahead), falling, rising)
        return jnp.where(j == chips - 1, z_me, chip)

    def section_of(i):
        return lax.rem(s_me + i, sections)

    def piece(r):
        return pl.ds(r * piece_rows, piece_rows)

    def pair_copy(b, j):
        return pltpu.make_async_remote_copy(
            src_ref=part.at[b, j, CORES - 1 - c_me], dst_ref=pair_in.at[b, j],
            send_sem=pair_send, recv_sem=pair_recv.at[b, j],
            device_id={"tensor": partner}, device_id_type=MESH,
        )

    def section_copy(b, i, j, r):
        return pltpu.make_async_remote_copy(
            src_ref=part.at[b, j, c_me, section_of(i), piece(r)],
            dst_ref=section_in.at[b, i - 1, j, piece(r)],
            send_sem=section_send, recv_sem=section_recv.at[b, i - 1, j, r],
            device_id={"section": section_of(i)}, device_id_type=MESH,
        )

    def chain_copy(b, j, r):
        chip = order(j)
        right = chip > z_me
        target = jnp.where(right, z_me + 1, z_me - 1)
        slot = jnp.where(right | (chip != target), chip, chips)
        return pltpu.make_async_remote_copy(
            src_ref=line_out.at[b, j, piece(r)], dst_ref=line_in.at[b, slot, piece(r)],
            send_sem=line_send, recv_sem=line_recv.at[b, slot, r],
            device_id={"tensor": target * CORES + c_me}, device_id_type=MESH,
        )

    def chain_wait(b, slot, r):
        pltpu.make_async_remote_copy(
            src_ref=line_out.at[b, 0, piece(r)], dst_ref=line_in.at[b, slot, piece(r)],
            send_sem=line_send, recv_sem=line_recv.at[b, slot, r],
            device_id={"tensor": partner}, device_id_type=MESH,
        ).wait_recv()

    def stat_copies(src, dst, send, recv):
        return [
            pltpu.make_async_remote_copy(
                src_ref=src, dst_ref=dst.at[i - 1],
                send_sem=send, recv_sem=recv,
                device_id={"tensor": lax.rem(t_me + i, tensors)}, device_id_type=MESH,
            )
            for i in range(1, tensors)
        ]

    def square_copies():
        return stat_copies(square_out, square_in, square_send, square_recv)

    def cross_copies(b):
        return stat_copies(
            cross_out.at[b], cross_in.at[b], cross_send, cross_recv.at[b]
        )

    def lane_sums(x):
        total = dot_nt(jnp.ones((8, feats), F32), x, lax.Precision.HIGHEST)
        return total[0:1, :]

    def spread(row):
        return dot_tn(
            jnp.broadcast_to(row, (8, rows)), jnp.full((8, feats), 0.125, F32),
            lax.Precision.HIGHEST,
        )

    def loop(low, high, step):
        def run(i, carry):
            step(i)
            return carry

        lax.fori_loop(low, high, run, 0)

    def project(b, j):
        width = CORES * feats
        block = dot_nt(
            grads[...], w_buf[pl.ds(pl.multiple_of(order(j) * width, width), width), :]
        )
        for half in range(CORES):
            part[b, j, half] = block[:, half * feats : (half + 1) * feats].reshape(
                sections, rows, feats
            )
        pair_copy(b, j).start()

    def send_section(b, j):
        pair_copy(b, j).wait_recv()
        for i in range(1, sections):
            section = section_of(i)
            for r in range(pieces):
                part[b, j, c_me, section, piece(r)] += pair_in[b, j, section, piece(r)]
                section_copy(b, i, j, r).start()

    lead = 1 if chips > 1 else 0

    def project_all(b, between):
        def step(j):
            project(b, j)

            @pl.when(j == 1)
            def _():
                send_section(b, 0)

            @pl.when(j >= 3)
            def _():
                send_section(b, j - 2)

            between(j)

        loop(0, chips, step)

    def send_rest(b):
        loop(max(lead, chips - 2), chips, lambda j: send_section(b, j))

    def gather_piece(b, j, r):
        total = part[b, j, c_me, s_me, piece(r)] + pair_in[b, j, s_me, piece(r)]
        for i in range(1, sections):
            section_copy(b, i, j, r).wait_recv()
            total = total + section_in[b, i - 1, j, piece(r)]
        line_out[b, j, piece(r)] = total
        chip = order(j)
        behind = jnp.where(chip > z_me, z_me > 0, z_me < chips - 1)

        @pl.when((j < chips - 1) & behind)
        def _():
            chain_wait(b, chip, r)
            line_out[b, j, piece(r)] += line_in[b, chip, piece(r)]

        @pl.when(j < chips - 1)
        def _():
            chain_copy(b, j, r).start()

    def finish_sum(b):
        own = chips - 1
        for r in range(pieces):
            @pl.when(z_me > 0)
            def _():
                chain_wait(b, z_me, r)
                line_out[b, own, piece(r)] += line_in[b, z_me, piece(r)]

            @pl.when(z_me < chips - 1)
            def _():
                chain_wait(b, chips, r)
                line_out[b, own, piece(r)] += line_in[b, chips, piece(r)]

            out_ref[b, piece(r)] = gain[...] * line_out[b, own, piece(r)]
        cross_out[b] = lane_sums(out_ref[b] * hidden[b])
        for copy in cross_copies(b):
            copy.start()
        out_ref[b] = out_ref[b] * inverse_wide[b]

    def prepare_norm():
        settle(square_in, square_recv)
        for b in range(seqs):
            square = square_out[b]
            for i in range(tensors - 1):
                square = square + square_in[i, b]
            inverse = lax.rsqrt(square / model_width + EPSILON)
            inverse_wide[b] = spread(inverse)
            hidden_scaled[b] = hidden[b] * spread(inverse * inverse * inverse / model_width)

    def finish_norm(b):
        cross = cross_out[b]
        settle(cross_in.at[b], cross_recv.at[b])
        for i in range(tensors - 1):
            cross = cross + cross_in[b, i]
        out_ref[b] = out_ref[b] - hidden_scaled[b] * spread(cross)

    steps = heads // 2
    total_pieces = chips * pieces

    def gather_span(b, low, high):
        def step(n):
            gather_piece(b, lax.div(n, pieces), lax.rem(n, pieces))

        loop(jnp.minimum(low, total_pieces), jnp.minimum(high, total_pieces), step)

    delay = jnp.where(at_end, 0, 3)
    batch = max(pieces // 2, 1)

    def gather_until(b, point):
        low = jnp.maximum(point - delay, 0) * batch
        high = jnp.maximum(point + 1 - delay, 0) * batch
        gather_span(b, low, jnp.minimum(high, total_pieces - batch))

    points = steps + chips

    def sequence(b):
        def heads_step(j):
            head_pair(b * heads + 2 * j)

            @pl.when((b == 0) & (j == 0))
            def _():
                pl.semaphore_wait(barrier, tensors - 1 + sections - 1)

            @pl.when(b > 0)
            def _():
                @pl.when(j == 0)
                def _():
                    send_rest(b - 1)

                gather_until(b - 1, j)

        def between(j):
            @pl.when(b > 0)
            def _():
                gather_until(b - 1, steps + j)

        loop(0, steps, heads_step)

        @pl.when(b == 0)
        def _():
            for copy in small_copies:
                copy.wait()
            settle(w_buf, weight_sem)

        project_all(b, between)

        @pl.when(b == 0)
        def _():
            for i in range(seqs):
                square_out[i] = lane_sums(hidden[i] * hidden[i])
            for copy in square_copies():
                copy.start()

    wait_loads(0)
    score_step(0, even)
    loop(0, seqs, sequence)
    last = seqs - 1
    send_rest(last)
    if seqs > 1:
        done = jnp.minimum(jnp.maximum(points - delay, 0) * batch, total_pieces - batch)
        gather_span(last - 1, done, total_pieces)
    prepare_norm()
    gather_span(last, 0, total_pieces // 2)
    for b in range(seqs - 1):
        finish_sum(b)
    gather_span(last, total_pieces // 2, total_pieces)
    finish_sum(last)
    for b in range(seqs):
        finish_norm(b)

    settle(pair_in, pair_send)
    settle(section_in, section_send)
    settle(line_out.at[:, pl.ds(0, chips - 1)], line_send)
    settle(square_in, square_send)
    settle(cross_in, cross_send)


def per_device(
    sections, tensors,
    dec_queries, enc_keys, enc_values, out_grad, key_weight, value_weight, enc_hidden, enc_gain,
):
    _, seqs, dec_len, inner = dec_queries.shape
    enc_len = enc_keys.shape[2]
    heads = inner // DK
    model_width = key_weight.shape[1]
    chips = tensors // CORES
    feats = model_width // tensors
    rows = enc_len // sections
    dma = pltpu.SemaphoreType.DMA
    query_block = min(QUERY_BLOCK, dec_len)
    blocks = dec_len // query_block
    unit = [
        pltpu.VMEM((blocks, enc_len, query_block), F32),
        pltpu.VMEM((blocks, enc_len, query_block), F32),
        pltpu.VMEM((blocks, 1, query_block), F32),
    ]
    call = pl.pallas_call(
        functools.partial(body, sections, tensors, query_block),
        out_shape=jax.ShapeDtypeStruct((seqs, rows, feats), F32),
        in_specs=[pl.BlockSpec(memory_space=pl.ANY)] * 8,
        out_specs=pl.BlockSpec(memory_space=pltpu.VMEM),
        scratch_shapes=[
            pltpu.VMEM((seqs, heads, 2, dec_len, DK), BF16),
            pltpu.VMEM((seqs, heads, 2, enc_len, DK), BF16),
            pltpu.VMEM((model_width, 2 * inner), BF16),
            pltpu.VMEM((seqs, rows, feats), F32),
            pltpu.VMEM((1, feats), F32),
            pltpu.VMEM((enc_len, 2 * inner), BF16),
            *unit, *unit,
            pltpu.VMEM((seqs, chips, CORES, sections, rows, feats), F32),
            pltpu.VMEM((seqs, chips, sections, rows, feats), F32),
            pltpu.VMEM((seqs, sections - 1, chips, rows, feats), F32),
            pltpu.VMEM((seqs, chips, rows, feats), F32),
            pltpu.VMEM((seqs, chips + 1, rows, feats), F32),
            pltpu.VMEM((seqs, 1, rows), F32),
            pltpu.VMEM((tensors - 1, seqs, 1, rows), F32),
            pltpu.VMEM((seqs, 1, rows), F32),
            pltpu.VMEM((seqs, tensors - 1, 1, rows), F32),
            pltpu.VMEM((seqs, rows, feats), F32),
            pltpu.VMEM((seqs, rows, feats), F32),
            dma((2, seqs, heads)),
            dma(()),
            dma((2,)),
            dma(()),
            dma((seqs, chips)),
            dma(()),
            dma((seqs, sections - 1, chips, PIECES)),
            dma(()),
            dma((seqs, chips + 1, PIECES)),
            dma(()),
            dma(()),
            dma(()),
            dma((seqs,)),
        ],
        compiler_params=pltpu.CompilerParams(
            collective_id=0, has_side_effects=True, vmem_limit_bytes=60 * 1024 * 1024
        ),
    )
    return call(
        dec_queries, enc_keys, enc_values, out_grad, key_weight, value_weight,
        enc_hidden, enc_gain.reshape(1, feats),
    )


def solution(mesh):
    wide = P("section", "dp", None, "tensor")
    return jax.shard_map(
        functools.partial(per_device, mesh.shape["section"], mesh.shape["tensor"]),
        mesh=mesh,
        in_specs=(
            wide, wide, wide, wide,
            P("section", None, "tensor"),
            P("section", None, "tensor"),
            P("dp", "section", "tensor"),
            P("tensor"),
        ),
        out_specs=P("dp", "section", "tensor"),
        check_vma=False,
    )
```

```python
import functools

import jax
import jax.numpy as jnp
from jax import lax
from jax.experimental import pallas as pl
from jax.experimental.pallas import tpu as pltpu
from jax.sharding import PartitionSpec as P

DK = 128
CORES = 2
EPSILON = 1e-06
MESH = pl.DeviceIdType.MESH
F32 = jnp.float32
BF16 = jnp.bfloat16
QUERY_BLOCK = 128
PIECES = 2


def dot_nt(a, b, precision=None):
    return lax.dot_general(
        a, b, (((1,), (1,)), ((), ())), precision=precision, preferred_element_type=F32
    )


def dot_nn(a, b):
    return lax.dot_general(a, b, (((1,), (0,)), ((), ())), preferred_element_type=F32)


def dot_tn(a, b, precision=None):
    return lax.dot_general(
        a, b, (((0,), (0,)), ((), ())), precision=precision, preferred_element_type=F32
    )


def body(
    sections, tensors, query_block,
    q_hbm, k_hbm, v_hbm, g_hbm, wk_hbm, wv_hbm, hidden_hbm, gain_hbm,
    out_ref,
    qg_buf, kv_buf, w_buf, hidden, gain, grads,
    scores_even, prob_grad_even, peak_even, scores_odd, prob_grad_odd, peak_odd,
    part, pair_in, section_in, line_out, line_in,
    square_out, square_in, cross_out, cross_in, inverse_gain, hidden_scaled, scaled_hidden, products,
    load_sem, weight_sem, small_sem,
    pair_send, pair_recv, section_send, section_recv, line_send, line_recv,
    square_send, square_recv, cross_send, cross_recv,
    share_send, share_recv,
):
    seqs, heads, _, dec_len, _ = qg_buf.shape
    enc_len = kv_buf.shape[3]
    inner = heads * DK
    model_width = w_buf.shape[0]
    feats = out_ref.shape[2]
    rows = out_ref.shape[1]
    chips = tensors // CORES
    s_me = lax.axis_index("section")
    t_me = lax.axis_index("tensor")
    z_me = lax.div(t_me, CORES)
    c_me = lax.rem(t_me, CORES)
    partner = z_me * CORES + (CORES - 1 - c_me)
    pieces = PIECES
    at_end = (z_me == 0) | (z_me == chips - 1)
    piece_rows = rows // pieces

    def loads(b, h):
        cols = pl.ds(pl.multiple_of(h * DK, DK), DK)
        return [
            pltpu.make_async_copy(src.at[0, b, :, cols], dst.at[b, h, n], load_sem.at[i, b, h])
            for i, (sources, dst) in enumerate((((q_hbm, g_hbm), qg_buf), ((k_hbm, v_hbm), kv_buf)))
            for n, src in enumerate(sources)
        ]

    def settle(ref, sem):
        pltpu.make_async_copy(ref, ref, sem).wait()

    def start_loads(b):
        def step(h, carry):
            for copy in loads(b, h):
                copy.start()
            return carry

        lax.fori_loop(0, heads, step, 0)

    weight_copies = [
        pltpu.make_async_copy(src.at[0], w_buf.at[:, pl.ds(i * inner, inner)], weight_sem)
        for i, src in enumerate((wk_hbm, wv_hbm))
    ]
    small_copies = [
        pltpu.make_async_copy(hidden_hbm, hidden, small_sem.at[0]),
        pltpu.make_async_copy(gain_hbm, gain, small_sem.at[1]),
    ]

    start_loads(0)
    for copy in small_copies + weight_copies:
        copy.start()
    for b in range(1, seqs):
        start_loads(b)

    barrier = pltpu.get_barrier_semaphore()
    for i in range(1, tensors):
        pl.semaphore_signal(
            barrier, inc=1, device_id={"tensor": lax.rem(t_me + i, tensors)}, device_id_type=MESH
        )
    for i in range(1, sections):
        pl.semaphore_signal(
            barrier, inc=1, device_id={"section": lax.rem(s_me + i, sections)}, device_id_type=MESH
        )

    blocks = dec_len // query_block

    def wait_loads(i):
        b, h = lax.div(i, heads), lax.rem(i, heads)
        settle(qg_buf.at[b, h], load_sem.at[0, b, h])
        settle(kv_buf.at[b, h], load_sem.at[1, b, h])

    def score_step(i, bufs):
        scores_buf, prob_grad_buf, peak_buf = bufs
        b, h = lax.div(i, heads), lax.rem(i, heads)
        keys = kv_buf[b, h, 0]
        values = kv_buf[b, h, 1]
        for n in range(blocks):
            span = pl.ds(n * query_block, query_block)
            scores = dot_nt(keys, qg_buf[b, h, 0, span, :])
            scores_buf[n] = scores
            peak_buf[n] = jnp.max(scores, axis=0, keepdims=True)
            prob_grad_buf[n] = dot_nt(values, qg_buf[b, h, 1, span, :])

    def grad_step(i, bufs):
        scores_buf, prob_grad_buf, peak_buf = bufs
        b, h = lax.div(i, heads), lax.rem(i, heads)
        key_grad = None
        for n in range(blocks):
            span = pl.ds(n * query_block, query_block)
            shifted = jnp.exp(scores_buf[n] - peak_buf[n])
            scale = 1.0 / jnp.sum(shifted, axis=0, keepdims=True)
            probs = shifted * scale
            probs_low = probs.astype(BF16)
            row_dot = jnp.sum(probs_low.astype(F32) * prob_grad_buf[n], axis=0, keepdims=True)
            score_low = (probs * (prob_grad_buf[n] - row_dot)).astype(BF16)
            value_term = dot_nn(probs_low, qg_buf[b, h, 1, span, :])
            key_term = dot_nn(score_low, qg_buf[b, h, 0, span, :])
            if key_grad is None:
                key_grad, value_grad = key_term, value_term
            else:
                key_grad, value_grad = key_grad + key_term, value_grad + value_term
        grads[:, pl.ds(pl.multiple_of(h * DK, DK), DK)] = key_grad.astype(BF16)
        grads[:, pl.ds(pl.multiple_of(inner + h * DK, DK), DK)] = value_grad.astype(BF16)

    even = (scores_even, prob_grad_even, peak_even)
    odd = (scores_odd, prob_grad_odd, peak_odd)

    def head_pair(i):
        wait_loads(i + 1)
        score_step(i + 1, odd)
        grad_step(i, even)
        following = jnp.minimum(i + 2, seqs * heads - 1)

        @pl.when(i + 2 < seqs * heads)
        def _():
            wait_loads(i + 2)

        score_step(following, even)
        grad_step(i + 1, odd)

    last = seqs - 1
    lower = z_me < chips // 2
    ahead = jnp.where(lower, chips - 1 - z_me, z_me)

    def order(j):
        rising = jnp.where(j < ahead, j, j - ahead)
        falling = chips - 1 - rising
        chip = jnp.where(lower == (j < ahead), falling, rising)
        return jnp.where(j == chips - 1, z_me, chip)

    def section_of(i):
        return lax.rem(s_me + i, sections)

    def piece(r):
        return pl.ds(r * piece_rows, piece_rows)

    def pair_copy(b, j):
        return pltpu.make_async_remote_copy(
            src_ref=part.at[b, j, CORES - 1 - c_me], dst_ref=pair_in.at[b, j],
            send_sem=pair_send, recv_sem=pair_recv.at[b, j],
            device_id={"tensor": partner}, device_id_type=MESH,
        )

    def section_copy(b, i, j, r):
        return pltpu.make_async_remote_copy(
            src_ref=part.at[b, j, c_me, section_of(i), piece(r)],
            dst_ref=section_in.at[b, i - 1, j, piece(r)],
            send_sem=section_send, recv_sem=section_recv.at[b, i - 1, j, r],
            device_id={"section": section_of(i)}, device_id_type=MESH,
        )

    def chain_copy(b, j, r):
        chip = order(j)
        right = chip > z_me
        target = jnp.where(right, z_me + 1, z_me - 1)
        slot = jnp.where(right | (chip != target), chip, chips)
        return pltpu.make_async_remote_copy(
            src_ref=line_out.at[b, j, piece(r)], dst_ref=line_in.at[b, slot, piece(r)],
            send_sem=line_send, recv_sem=line_recv.at[b, slot, r],
            device_id={"tensor": target * CORES + c_me}, device_id_type=MESH,
        )

    def chain_wait(b, slot, r):
        pltpu.make_async_remote_copy(
            src_ref=line_out.at[b, 0, piece(r)], dst_ref=line_in.at[b, slot, piece(r)],
            send_sem=line_send, recv_sem=line_recv.at[b, slot, r],
            device_id={"tensor": partner}, device_id_type=MESH,
        ).wait_recv()

    def share_copy(i):
        return pltpu.make_async_remote_copy(
            src_ref=scaled_hidden.at[z_me], dst_ref=scaled_hidden.at[z_me],
            send_sem=share_send, recv_sem=share_recv,
            device_id={"tensor": lax.rem(z_me + i, chips) * CORES + c_me}, device_id_type=MESH,
        )

    def stat_copies(src, dst, send, recv):
        return [
            pltpu.make_async_remote_copy(
                src_ref=src, dst_ref=dst.at[i - 1],
                send_sem=send, recv_sem=recv,
                device_id={"tensor": lax.rem(t_me + i, tensors)}, device_id_type=MESH,
            )
            for i in range(1, tensors)
        ]

    def square_copies():
        return stat_copies(square_out, square_in, square_send, square_recv)

    def cross_copies(b):
        return stat_copies(
            cross_out.at[b], cross_in.at[b], cross_send, cross_recv.at[b]
        )

    def lane_sums(x):
        total = dot_nt(jnp.ones((8, feats), F32), x, lax.Precision.HIGHEST)
        return total[0:1, :]

    def spread(row):
        return dot_tn(
            jnp.broadcast_to(row, (8, rows)), jnp.full((8, feats), 0.125, F32),
            lax.Precision.HIGHEST,
        )

    def loop(low, high, step):
        def run(i, carry):
            step(i)
            return carry

        lax.fori_loop(low, high, run, 0)

    def project(b, j):
        width = CORES * feats
        block = dot_nt(
            grads[...], w_buf[pl.ds(pl.multiple_of(order(j) * width, width), width), :]
        )
        for half in range(CORES):
            part[b, j, half] = block[:, half * feats : (half + 1) * feats].reshape(
                sections, rows, feats
            )
        pair_copy(b, j).start()

    def send_section(b, j):
        pair_copy(b, j).wait_recv()
        for i in range(1, sections):
            section = section_of(i)
            for r in range(pieces):
                part[b, j, c_me, section, piece(r)] += pair_in[b, j, section, piece(r)]
                section_copy(b, i, j, r).start()

    lead = 1 if chips > 1 else 0

    def project_all(b, between):
        def step(j):
            project(b, j)

            @pl.when(j == 1)
            def _():
                send_section(b, 0)

            @pl.when(j >= 3)
            def _():
                send_section(b, j - 2)

            between(j)

        loop(0, chips, step)

    def send_rest(b):
        loop(max(lead, chips - 2), chips, lambda j: send_section(b, j))

    def gather_piece(b, j, r, tally=False):
        total = part[b, j, c_me, s_me, piece(r)] + pair_in[b, j, s_me, piece(r)]
        for i in range(1, sections):
            section_copy(b, i, j, r).wait_recv()
            total = total + section_in[b, i - 1, j, piece(r)]
        line_out[b, j, piece(r)] = total
        chip = order(j)
        if tally:
            products[piece(r)] += scaled_hidden[chip, piece(r)] * total
        behind = jnp.where(chip > z_me, z_me > 0, z_me < chips - 1)

        @pl.when((j < chips - 1) & behind)
        def _():
            chain_wait(b, chip, r)
            line_out[b, j, piece(r)] += line_in[b, chip, piece(r)]

        @pl.when(j < chips - 1)
        def _():
            chain_copy(b, j, r).start()

    def finish_sum(b):
        own = chips - 1
        for r in range(pieces):
            @pl.when(z_me > 0)
            def _():
                chain_wait(b, z_me, r)
                line_out[b, own, piece(r)] += line_in[b, z_me, piece(r)]

            @pl.when(z_me < chips - 1)
            def _():
                chain_wait(b, chips, r)
                line_out[b, own, piece(r)] += line_in[b, chips, piece(r)]

            out_ref[b, piece(r)] = line_out[b, own, piece(r)] * inverse_gain[b, piece(r)]

    def send_cross(b, terms):
        cross_out[b] = lane_sums(terms)
        for copy in cross_copies(b):
            copy.start()

    def prepare_norm():
        settle(square_in, square_recv)
        settle(scaled_hidden.at[pl.ds(0, chips - 1)], share_recv)
        products[...] = jnp.zeros_like(products)
        for b in range(seqs):
            square = square_out[b]
            for i in range(tensors - 1):
                square = square + square_in[i, b]
            inverse = lax.rsqrt(square / model_width + EPSILON)
            inverse_gain[b] = gain[...] * spread(inverse)
            hidden_scaled[b] = hidden[b] * spread(inverse * inverse * inverse / model_width)

    def finish_norm(b):
        cross = cross_out[b]
        settle(cross_in.at[b], cross_recv.at[b])
        for i in range(tensors - 1):
            cross = cross + cross_in[b, i]
        out_ref[b] = out_ref[b] - hidden_scaled[b] * spread(cross)

    steps = heads // 2
    total_pieces = chips * pieces

    def gather_span(b, low, high, tally=False):
        def step(n):
            gather_piece(b, lax.div(n, pieces), lax.rem(n, pieces), tally)

        loop(jnp.minimum(low, total_pieces), jnp.minimum(high, total_pieces), step)

    delay = jnp.where(at_end, 0, 3)
    batch = max(pieces // 2, 1)

    def gather_until(b, point):
        low = jnp.maximum(point - delay, 0) * batch
        high = jnp.maximum(point + 1 - delay, 0) * batch
        gather_span(b, low, jnp.minimum(high, total_pieces - batch))

    points = steps + chips

    def sequence(b):
        def heads_step(j):
            head_pair(b * heads + 2 * j)

            @pl.when((b == 0) & (j == 0))
            def _():
                for copy in small_copies:
                    copy.wait()
                scaled_hidden[z_me] = gain[...] * hidden[last]
                pl.semaphore_wait(barrier, tensors - 1 + sections - 1)
                for i in range(1, chips):
                    share_copy(i).start()

            @pl.when(b > 0)
            def _():
                @pl.when(j == 0)
                def _():
                    send_rest(b - 1)

                gather_until(b - 1, j)

        def between(j):
            @pl.when(b > 0)
            def _():
                gather_until(b - 1, steps + j)

        loop(0, steps, heads_step)

        @pl.when(b == 0)
        def _():
            settle(w_buf, weight_sem)

        project_all(b, between)

        @pl.when(b == 0)
        def _():
            for i in range(seqs):
                square_out[i] = lane_sums(hidden[i] * hidden[i])
            for copy in square_copies():
                copy.start()

    wait_loads(0)
    score_step(0, even)
    loop(0, seqs, sequence)
    send_rest(last)
    if seqs > 1:
        done = jnp.minimum(jnp.maximum(points - delay, 0) * batch, total_pieces - batch)
        gather_span(last - 1, done, total_pieces)
    prepare_norm()
    gather_span(last, 0, total_pieces // 2, True)
    for b in range(last):
        finish_sum(b)
        send_cross(b, line_out[b, chips - 1] * (gain[...] * hidden[b]))
    gather_span(last, total_pieces // 2, total_pieces, True)
    send_cross(last, products[...])
    finish_sum(last)
    for b in range(seqs):
        finish_norm(b)

    settle(pair_in, pair_send)
    settle(section_in, section_send)
    settle(line_out.at[:, pl.ds(0, chips - 1)], line_send)
    settle(square_in, square_send)
    settle(cross_in, cross_send)
    settle(scaled_hidden.at[pl.ds(0, chips - 1)], share_send)


def per_device(
    sections, tensors,
    dec_queries, enc_keys, enc_values, out_grad, key_weight, value_weight, enc_hidden, enc_gain,
):
    _, seqs, dec_len, inner = dec_queries.shape
    enc_len = enc_keys.shape[2]
    heads = inner // DK
    model_width = key_weight.shape[1]
    chips = tensors // CORES
    feats = model_width // tensors
    rows = enc_len // sections
    dma = pltpu.SemaphoreType.DMA
    query_block = min(QUERY_BLOCK, dec_len)
    blocks = dec_len // query_block
    unit = [
        pltpu.VMEM((blocks, enc_len, query_block), F32),
        pltpu.VMEM((blocks, enc_len, query_block), F32),
        pltpu.VMEM((blocks, 1, query_block), F32),
    ]
    call = pl.pallas_call(
        functools.partial(body, sections, tensors, query_block),
        out_shape=jax.ShapeDtypeStruct((seqs, rows, feats), F32),
        in_specs=[pl.BlockSpec(memory_space=pl.ANY)] * 8,
        out_specs=pl.BlockSpec(memory_space=pltpu.VMEM),
        scratch_shapes=[
            pltpu.VMEM((seqs, heads, 2, dec_len, DK), BF16),
            pltpu.VMEM((seqs, heads, 2, enc_len, DK), BF16),
            pltpu.VMEM((model_width, 2 * inner), BF16),
            pltpu.VMEM((seqs, rows, feats), F32),
            pltpu.VMEM((1, feats), F32),
            pltpu.VMEM((enc_len, 2 * inner), BF16),
            *unit, *unit,
            pltpu.VMEM((seqs, chips, CORES, sections, rows, feats), F32),
            pltpu.VMEM((seqs, chips, sections, rows, feats), F32),
            pltpu.VMEM((seqs, sections - 1, chips, rows, feats), F32),
            pltpu.VMEM((seqs, chips, rows, feats), F32),
            pltpu.VMEM((seqs, chips + 1, rows, feats), F32),
            pltpu.VMEM((seqs, 1, rows), F32),
            pltpu.VMEM((tensors - 1, seqs, 1, rows), F32),
            pltpu.VMEM((seqs, 1, rows), F32),
            pltpu.VMEM((seqs, tensors - 1, 1, rows), F32),
            pltpu.VMEM((seqs, rows, feats), F32),
            pltpu.VMEM((seqs, rows, feats), F32),
            pltpu.VMEM((chips, rows, feats), F32),
            pltpu.VMEM((rows, feats), F32),
            dma((2, seqs, heads)),
            dma(()),
            dma((2,)),
            dma(()),
            dma((seqs, chips)),
            dma(()),
            dma((seqs, sections - 1, chips, PIECES)),
            dma(()),
            dma((seqs, chips + 1, PIECES)),
            dma(()),
            dma(()),
            dma(()),
            dma((seqs,)),
            dma(()),
            dma(()),
        ],
        compiler_params=pltpu.CompilerParams(
            collective_id=0, has_side_effects=True, vmem_limit_bytes=60 * 1024 * 1024
        ),
    )
    return call(
        dec_queries, enc_keys, enc_values, out_grad, key_weight, value_weight,
        enc_hidden, enc_gain.reshape(1, feats),
    )


def solution(mesh):
    wide = P("section", "dp", None, "tensor")
    return jax.shard_map(
        functools.partial(per_device, mesh.shape["section"], mesh.shape["tensor"]),
        mesh=mesh,
        in_specs=(
            wide, wide, wide, wide,
            P("section", None, "tensor"),
            P("section", None, "tensor"),
            P("dp", "section", "tensor"),
            P("tensor"),
        ),
        out_specs=P("dp", "section", "tensor"),
        check_vma=False,
    )
```

```python
import functools

import jax
import jax.numpy as jnp
from jax import lax
from jax.experimental import pallas as pl
from jax.experimental.pallas import tpu as pltpu
from jax.sharding import PartitionSpec as P

DK = 128
CORES = 2
EPSILON = 1e-06
MESH = pl.DeviceIdType.MESH
F32 = jnp.float32
BF16 = jnp.bfloat16
QUERY_BLOCK = 128
PIECES = 2


def dot_nt(a, b, precision=None):
    return lax.dot_general(
        a, b, (((1,), (1,)), ((), ())), precision=precision, preferred_element_type=F32
    )


def dot_nn(a, b):
    return lax.dot_general(a, b, (((1,), (0,)), ((), ())), preferred_element_type=F32)


def dot_tn(a, b, precision=None):
    return lax.dot_general(
        a, b, (((0,), (0,)), ((), ())), precision=precision, preferred_element_type=F32
    )


def body(
    sections, tensors, query_block,
    q_hbm, k_hbm, v_hbm, g_hbm, wk_hbm, wv_hbm, hidden_hbm, gain_hbm,
    out_ref,
    qg_buf, kv_buf, w_buf, hidden, gain, grads,
    scores_even, prob_grad_even, peak_even, scores_odd, prob_grad_odd, peak_odd,
    part, pair_in, section_in, line_out, line_in,
    square_out, square_in, cross_out, cross_in, inverse_gain, hidden_scaled, scaled_hidden, products,
    load_sem, weight_sem, small_sem,
    pair_send, pair_recv, section_send, section_recv, line_send, line_recv,
    square_send, square_recv, cross_send, cross_recv,
    share_send, share_recv,
):
    seqs, heads, _, dec_len, _ = qg_buf.shape
    enc_len = kv_buf.shape[3]
    inner = heads * DK
    model_width = w_buf.shape[0]
    feats = out_ref.shape[2]
    rows = out_ref.shape[1]
    chips = tensors // CORES
    s_me = lax.axis_index("section")
    t_me = lax.axis_index("tensor")
    z_me = lax.div(t_me, CORES)
    c_me = lax.rem(t_me, CORES)
    partner = z_me * CORES + (CORES - 1 - c_me)
    pieces = PIECES
    at_end = (z_me == 0) | (z_me == chips - 1)
    piece_rows = rows // pieces

    def loads(b, h):
        cols = pl.ds(pl.multiple_of(h * DK, DK), DK)
        return [
            pltpu.make_async_copy(src.at[0, b, :, cols], dst.at[b, h, n], load_sem.at[i, b, h])
            for i, (sources, dst) in enumerate((((q_hbm, g_hbm), qg_buf), ((k_hbm, v_hbm), kv_buf)))
            for n, src in enumerate(sources)
        ]

    def settle(ref, sem):
        pltpu.make_async_copy(ref, ref, sem).wait()

    def start_loads(b):
        def step(h, carry):
            for copy in loads(b, h):
                copy.start()
            return carry

        lax.fori_loop(0, heads, step, 0)

    weight_copies = [
        pltpu.make_async_copy(src.at[0], w_buf.at[:, pl.ds(i * inner, inner)], weight_sem)
        for i, src in enumerate((wk_hbm, wv_hbm))
    ]
    small_copies = [
        pltpu.make_async_copy(hidden_hbm, hidden, small_sem.at[0]),
        pltpu.make_async_copy(gain_hbm, gain, small_sem.at[1]),
    ]

    start_loads(0)
    for copy in small_copies + weight_copies:
        copy.start()
    for b in range(1, seqs):
        start_loads(b)

    barrier = pltpu.get_barrier_semaphore()
    for i in range(1, tensors):
        pl.semaphore_signal(
            barrier, inc=1, device_id={"tensor": lax.rem(t_me + i, tensors)}, device_id_type=MESH
        )
    for i in range(1, sections):
        pl.semaphore_signal(
            barrier, inc=1, device_id={"section": lax.rem(s_me + i, sections)}, device_id_type=MESH
        )

    blocks = dec_len // query_block

    def wait_loads(i):
        b, h = lax.div(i, heads), lax.rem(i, heads)
        settle(qg_buf.at[b, h], load_sem.at[0, b, h])
        settle(kv_buf.at[b, h], load_sem.at[1, b, h])

    def score_step(i, bufs):
        scores_buf, prob_grad_buf, peak_buf = bufs
        b, h = lax.div(i, heads), lax.rem(i, heads)
        keys = kv_buf[b, h, 0]
        values = kv_buf[b, h, 1]
        for n in range(blocks):
            span = pl.ds(n * query_block, query_block)
            scores = dot_nt(keys, qg_buf[b, h, 0, span, :])
            scores_buf[n] = scores
            peak_buf[n] = jnp.max(scores, axis=0, keepdims=True)
            prob_grad_buf[n] = dot_nt(values, qg_buf[b, h, 1, span, :])

    def grad_step(i, bufs):
        scores_buf, prob_grad_buf, peak_buf = bufs
        b, h = lax.div(i, heads), lax.rem(i, heads)
        key_grad = None
        for n in range(blocks):
            span = pl.ds(n * query_block, query_block)
            shifted = jnp.exp(scores_buf[n] - peak_buf[n])
            scale = 1.0 / jnp.sum(shifted, axis=0, keepdims=True)
            probs = shifted * scale
            probs_low = probs.astype(BF16)
            row_dot = jnp.sum(probs_low.astype(F32) * prob_grad_buf[n], axis=0, keepdims=True)
            score_low = (probs * (prob_grad_buf[n] - row_dot)).astype(BF16)
            value_term = dot_nn(probs_low, qg_buf[b, h, 1, span, :])
            key_term = dot_nn(score_low, qg_buf[b, h, 0, span, :])
            if key_grad is None:
                key_grad, value_grad = key_term, value_term
            else:
                key_grad, value_grad = key_grad + key_term, value_grad + value_term
        grads[:, pl.ds(pl.multiple_of(h * DK, DK), DK)] = key_grad.astype(BF16)
        grads[:, pl.ds(pl.multiple_of(inner + h * DK, DK), DK)] = value_grad.astype(BF16)

    even = (scores_even, prob_grad_even, peak_even)
    odd = (scores_odd, prob_grad_odd, peak_odd)

    def head_pair(i):
        wait_loads(i + 1)
        score_step(i + 1, odd)
        grad_step(i, even)
        following = jnp.minimum(i + 2, seqs * heads - 1)

        @pl.when(i + 2 < seqs * heads)
        def _():
            wait_loads(i + 2)

        score_step(following, even)
        grad_step(i + 1, odd)

    last = seqs - 1
    lower = z_me < chips // 2
    ahead = jnp.where(lower, chips - 1 - z_me, z_me)

    def order(j):
        rising = jnp.where(j < ahead, j, j - ahead)
        falling = chips - 1 - rising
        chip = jnp.where(lower == (j < ahead), falling, rising)
        return jnp.where(j == chips - 1, z_me, chip)

    def section_of(i):
        return lax.rem(s_me + i, sections)

    def piece(r):
        return pl.ds(r * piece_rows, piece_rows)

    def pair_copy(b, j):
        return pltpu.make_async_remote_copy(
            src_ref=part.at[b, j, CORES - 1 - c_me], dst_ref=pair_in.at[b, j],
            send_sem=pair_send, recv_sem=pair_recv.at[b, j],
            device_id={"tensor": partner}, device_id_type=MESH,
        )

    def section_copy(b, i, j, r):
        return pltpu.make_async_remote_copy(
            src_ref=part.at[b, j, c_me, section_of(i), piece(r)],
            dst_ref=section_in.at[b, i - 1, j, piece(r)],
            send_sem=section_send, recv_sem=section_recv.at[b, i - 1, j, r],
            device_id={"section": section_of(i)}, device_id_type=MESH,
        )

    def chain_copy(b, j, r):
        chip = order(j)
        right = chip > z_me
        target = jnp.where(right, z_me + 1, z_me - 1)
        slot = jnp.where(right | (chip != target), chip, chips)
        return pltpu.make_async_remote_copy(
            src_ref=line_out.at[b, j, piece(r)], dst_ref=line_in.at[b, slot, piece(r)],
            send_sem=line_send, recv_sem=line_recv.at[b, slot, r],
            device_id={"tensor": target * CORES + c_me}, device_id_type=MESH,
        )

    def chain_wait(b, slot, r):
        pltpu.make_async_remote_copy(
            src_ref=line_out.at[b, 0, piece(r)], dst_ref=line_in.at[b, slot, piece(r)],
            send_sem=line_send, recv_sem=line_recv.at[b, slot, r],
            device_id={"tensor": partner}, device_id_type=MESH,
        ).wait_recv()

    def share_copy(i):
        return pltpu.make_async_remote_copy(
            src_ref=scaled_hidden.at[z_me], dst_ref=scaled_hidden.at[z_me],
            send_sem=share_send, recv_sem=share_recv,
            device_id={"tensor": lax.rem(z_me + i, chips) * CORES + c_me}, device_id_type=MESH,
        )

    def stat_copies(src, dst, send, recv):
        return [
            pltpu.make_async_remote_copy(
                src_ref=src, dst_ref=dst.at[i - 1],
                send_sem=send, recv_sem=recv,
                device_id={"tensor": lax.rem(t_me + i, tensors)}, device_id_type=MESH,
            )
            for i in range(1, tensors)
        ]

    def square_copies():
        return stat_copies(square_out, square_in, square_send, square_recv)

    def cross_copies(b):
        return stat_copies(
            cross_out.at[b], cross_in.at[b], cross_send, cross_recv.at[b]
        )

    def lane_sums(x):
        total = dot_nt(jnp.ones((8, feats), F32), x, lax.Precision.HIGHEST)
        return total[0:1, :]

    def spread(row):
        return dot_tn(
            jnp.broadcast_to(row, (8, rows)), jnp.full((8, feats), 0.125, F32),
            lax.Precision.HIGHEST,
        )

    def loop(low, high, step):
        def run(i, carry):
            step(i)
            return carry

        lax.fori_loop(low, high, run, 0)

    def project(b, j):
        width = CORES * feats
        block = dot_nt(
            grads[...], w_buf[pl.ds(pl.multiple_of(order(j) * width, width), width), :]
        )
        for half in range(CORES):
            part[b, j, half] = block[:, half * feats : (half + 1) * feats].reshape(
                sections, rows, feats
            )
        pair_copy(b, j).start()

    def send_section(b, j):
        pair_copy(b, j).wait_recv()
        for i in range(1, sections):
            section = section_of(i)
            for r in range(pieces):
                part[b, j, c_me, section, piece(r)] += pair_in[b, j, section, piece(r)]
                section_copy(b, i, j, r).start()

    lead = 1 if chips > 1 else 0

    def project_all(b, between):
        def step(j):
            project(b, j)

            @pl.when(j == 1)
            def _():
                send_section(b, 0)

            @pl.when(j >= 3)
            def _():
                send_section(b, j - 2)

            between(j)

        loop(0, chips, step)

    def send_rest(b):
        loop(max(lead, chips - 2), chips, lambda j: send_section(b, j))

    def gather_piece(b, j, r, tally=False):
        total = part[b, j, c_me, s_me, piece(r)] + pair_in[b, j, s_me, piece(r)]
        for i in range(1, sections):
            section_copy(b, i, j, r).wait_recv()
            total = total + section_in[b, i - 1, j, piece(r)]
        line_out[b, j, piece(r)] = total
        chip = order(j)
        if tally:
            products[piece(r)] += scaled_hidden[chip, piece(r)] * total
        behind = jnp.where(chip > z_me, z_me > 0, z_me < chips - 1)

        @pl.when((j < chips - 1) & behind)
        def _():
            chain_wait(b, chip, r)
            line_out[b, j, piece(r)] += line_in[b, chip, piece(r)]

        @pl.when(j < chips - 1)
        def _():
            chain_copy(b, j, r).start()

    def finish_sum(b):
        own = chips - 1
        for r in range(pieces):
            @pl.when(z_me > 0)
            def _():
                chain_wait(b, z_me, r)
                line_out[b, own, piece(r)] += line_in[b, z_me, piece(r)]

            @pl.when(z_me < chips - 1)
            def _():
                chain_wait(b, chips, r)
                line_out[b, own, piece(r)] += line_in[b, chips, piece(r)]

            out_ref[b, piece(r)] = line_out[b, own, piece(r)] * inverse_gain[b, piece(r)]

    def send_cross(b, terms):
        cross_out[b] = lane_sums(terms)
        for copy in cross_copies(b):
            copy.start()

    def prepare_norm():
        settle(square_in, square_recv)
        settle(scaled_hidden.at[pl.ds(0, chips - 1)], share_recv)
        products[...] = jnp.zeros_like(products)
        for b in range(seqs):
            square = square_out[b]
            for i in range(tensors - 1):
                square = square + square_in[i, b]
            inverse = lax.rsqrt(square / model_width + EPSILON)
            inverse_gain[b] = gain[...] * spread(inverse)
            hidden_scaled[b] = hidden[b] * spread(inverse * inverse * inverse / model_width)

    def finish_norm(b):
        cross = cross_out[b]
        settle(cross_in.at[b], cross_recv.at[b])
        for i in range(tensors - 1):
            cross = cross + cross_in[b, i]
        out_ref[b] = out_ref[b] - hidden_scaled[b] * spread(cross)

    steps = heads // 2
    total_pieces = chips * pieces

    def gather_span(b, low, high, tally=False):
        def step(n):
            gather_piece(b, lax.div(n, pieces), lax.rem(n, pieces), tally)

        loop(jnp.minimum(low, total_pieces), jnp.minimum(high, total_pieces), step)

    delay = jnp.where(at_end, 0, 3)
    batch = max(pieces // 2, 1)

    def gather_until(b, point):
        low = jnp.maximum(point - delay, 0) * batch
        high = jnp.maximum(point + 1 - delay, 0) * batch
        gather_span(b, low, jnp.minimum(high, total_pieces - batch))

    points = steps + chips

    def sequence(b):
        def heads_step(j):
            head_pair(b * heads + 2 * j)

            @pl.when((b == 0) & (j == 0))
            def _():
                for copy in small_copies:
                    copy.wait()
                scaled_hidden[z_me] = gain[...] * hidden[last]
                pl.semaphore_wait(barrier, tensors - 1 + sections - 1)
                for i in range(1, chips):
                    share_copy(i).start()

            @pl.when(b > 0)
            def _():
                @pl.when(j == 0)
                def _():
                    send_rest(b - 1)

                gather_until(b - 1, j)

        def between(j):
            @pl.when(b > 0)
            def _():
                gather_until(b - 1, steps + j)

        loop(0, steps, heads_step)

        @pl.when(b == 0)
        def _():
            settle(w_buf, weight_sem)

        project_all(b, between)

        @pl.when(b == 0)
        def _():
            for i in range(seqs):
                square_out[i] = lane_sums(hidden[i] * hidden[i])
            for copy in square_copies():
                copy.start()

    wait_loads(0)
    score_step(0, even)
    loop(0, seqs, sequence)
    send_rest(last)
    if seqs > 1:
        done = jnp.minimum(jnp.maximum(points - delay, 0) * batch, total_pieces - batch)
        gather_span(last - 1, done, total_pieces)
    prepare_norm()
    gather_span(last, 0, total_pieces // 2, True)
    for b in range(last):
        finish_sum(b)
        send_cross(b, line_out[b, chips - 1] * (gain[...] * hidden[b]))
    gather_span(last, total_pieces // 2, total_pieces, True)
    send_cross(last, products[...])
    finish_sum(last)
    for b in range(seqs):
        finish_norm(b)

    settle(pair_in, pair_send)
    settle(section_in, section_send)
    settle(line_out.at[:, pl.ds(0, chips - 1)], line_send)
    settle(square_in, square_send)
    settle(cross_in, cross_send)
    settle(scaled_hidden.at[pl.ds(0, chips - 1)], share_send)


def per_device(
    sections, tensors,
    dec_queries, enc_keys, enc_values, out_grad, key_weight, value_weight, enc_hidden, enc_gain,
):
    _, seqs, dec_len, inner = dec_queries.shape
    enc_len = enc_keys.shape[2]
    heads = inner // DK
    model_width = key_weight.shape[1]
    chips = tensors // CORES
    feats = model_width // tensors
    rows = enc_len // sections
    dma = pltpu.SemaphoreType.DMA
    query_block = min(QUERY_BLOCK, dec_len)
    blocks = dec_len // query_block
    unit = [
        pltpu.VMEM((blocks, enc_len, query_block), F32),
        pltpu.VMEM((blocks, enc_len, query_block), F32),
        pltpu.VMEM((blocks, 1, query_block), F32),
    ]
    call = pl.pallas_call(
        functools.partial(body, sections, tensors, query_block),
        out_shape=jax.ShapeDtypeStruct((seqs, rows, feats), F32),
        in_specs=[pl.BlockSpec(memory_space=pl.ANY)] * 8,
        out_specs=pl.BlockSpec(memory_space=pltpu.VMEM),
        scratch_shapes=[
            pltpu.VMEM((seqs, heads, 2, dec_len, DK), BF16),
            pltpu.VMEM((seqs, heads, 2, enc_len, DK), BF16),
            pltpu.VMEM((model_width, 2 * inner), BF16),
            pltpu.VMEM((seqs, rows, feats), F32),
            pltpu.VMEM((1, feats), F32),
            pltpu.VMEM((enc_len, 2 * inner), BF16),
            *unit, *unit,
            pltpu.VMEM((seqs, chips, CORES, sections, rows, feats), F32),
            pltpu.VMEM((seqs, chips, sections, rows, feats), F32),
            pltpu.VMEM((seqs, sections - 1, chips, rows, feats), F32),
            pltpu.VMEM((seqs, chips, rows, feats), F32),
            pltpu.VMEM((seqs, chips + 1, rows, feats), F32),
            pltpu.VMEM((seqs, 1, rows), F32),
            pltpu.VMEM((tensors - 1, seqs, 1, rows), F32),
            pltpu.VMEM((seqs, 1, rows), F32),
            pltpu.VMEM((seqs, tensors - 1, 1, rows), F32),
            pltpu.VMEM((seqs, rows, feats), F32),
            pltpu.VMEM((seqs, rows, feats), F32),
            pltpu.VMEM((chips, rows, feats), F32),
            pltpu.VMEM((rows, feats), F32),
            dma((2, seqs, heads)),
            dma(()),
            dma((2,)),
            dma(()),
            dma((seqs, chips)),
            dma(()),
            dma((seqs, sections - 1, chips, PIECES)),
            dma(()),
            dma((seqs, chips + 1, PIECES)),
            dma(()),
            dma(()),
            dma(()),
            dma((seqs,)),
            dma(()),
            dma(()),
        ],
        compiler_params=pltpu.CompilerParams(
            collective_id=0, has_side_effects=True, vmem_limit_bytes=48 * 1024 * 1024
        ),
    )
    operands = (
        dec_queries, enc_keys, enc_values, out_grad, key_weight, value_weight,
        enc_hidden, enc_gain.reshape(1, feats),
    )
    return call(*(pltpu.with_memory_space_constraint(x, pltpu.HBM) for x in operands))


def solution(mesh):
    wide = P("section", "dp", None, "tensor")
    return jax.shard_map(
        functools.partial(per_device, mesh.shape["section"], mesh.shape["tensor"]),
        mesh=mesh,
        in_specs=(
            wide, wide, wide, wide,
            P("section", None, "tensor"),
            P("section", None, "tensor"),
            P("dp", "section", "tensor"),
            P("tensor"),
        ),
        out_specs=P("dp", "section", "tensor"),
        check_vma=False,
    )
```

```python
import functools

import jax
import jax.numpy as jnp
from jax import lax
from jax.experimental import pallas as pl
from jax.experimental.pallas import tpu as pltpu
from jax.sharding import PartitionSpec as P

DK = 128
CORES = 2
EPSILON = 1e-06
MESH = pl.DeviceIdType.MESH
F32 = jnp.float32
BF16 = jnp.bfloat16
QUERY_BLOCK = 128
PIECES = 2


def dot_nt(a, b, precision=None):
    return lax.dot_general(
        a, b, (((1,), (1,)), ((), ())), precision=precision, preferred_element_type=F32
    )


def dot_nn(a, b):
    return lax.dot_general(a, b, (((1,), (0,)), ((), ())), preferred_element_type=F32)


def dot_tn(a, b, precision=None):
    return lax.dot_general(
        a, b, (((0,), (0,)), ((), ())), precision=precision, preferred_element_type=F32
    )


def body(
    sections, tensors, query_block,
    q_hbm, k_hbm, v_hbm, g_hbm, wk_hbm, wv_hbm, hidden_hbm, gain_hbm,
    out_ref,
    qg_buf, kv_buf, w_buf, hidden, gain, grads,
    scores_even, prob_grad_even, peak_even, scores_odd, prob_grad_odd, peak_odd,
    part, pair_in, section_in, line_out, line_in,
    square_out, square_in, cross_out, cross_in, inverse_gain, hidden_scaled, scaled_hidden, products,
    load_sem, weight_sem, small_sem,
    pair_send, pair_recv, section_send, section_recv, line_send, line_recv,
    square_send, square_recv, cross_send, cross_recv,
    share_send, share_recv,
):
    seqs, heads, _, dec_len, _ = qg_buf.shape
    enc_len = kv_buf.shape[3]
    inner = heads * DK
    model_width = w_buf.shape[0]
    feats = out_ref.shape[2]
    rows = out_ref.shape[1]
    chips = tensors // CORES
    s_me = lax.axis_index("section")
    t_me = lax.axis_index("tensor")
    z_me = lax.div(t_me, CORES)
    c_me = lax.rem(t_me, CORES)
    partner = z_me * CORES + (CORES - 1 - c_me)
    pieces = PIECES
    at_end = (z_me == 0) | (z_me == chips - 1)
    piece_rows = rows // pieces

    def loads(b, h):
        cols = pl.ds(pl.multiple_of(h * DK, DK), DK)
        return [
            pltpu.make_async_copy(src.at[0, b, :, cols], dst.at[b, h, n], load_sem.at[i, b, h])
            for i, (sources, dst) in enumerate((((q_hbm, g_hbm), qg_buf), ((k_hbm, v_hbm), kv_buf)))
            for n, src in enumerate(sources)
        ]

    def settle(ref, sem):
        pltpu.make_async_copy(ref, ref, sem).wait()

    def start_loads(b):
        def step(h, carry):
            for copy in loads(b, h):
                copy.start()
            return carry

        lax.fori_loop(0, heads, step, 0)

    weight_copies = [
        pltpu.make_async_copy(src.at[0], w_buf.at[:, pl.ds(i * inner, inner)], weight_sem)
        for i, src in enumerate((wk_hbm, wv_hbm))
    ]
    small_copies = [
        pltpu.make_async_copy(hidden_hbm, hidden, small_sem.at[0]),
        pltpu.make_async_copy(gain_hbm, gain, small_sem.at[1]),
    ]

    start_loads(0)
    for copy in small_copies + weight_copies:
        copy.start()
    for b in range(1, seqs):
        start_loads(b)

    barrier = pltpu.get_barrier_semaphore()
    for i in range(1, tensors):
        pl.semaphore_signal(
            barrier, inc=1, device_id={"tensor": lax.rem(t_me + i, tensors)}, device_id_type=MESH
        )
    for i in range(1, sections):
        pl.semaphore_signal(
            barrier, inc=1, device_id={"section": lax.rem(s_me + i, sections)}, device_id_type=MESH
        )

    blocks = dec_len // query_block

    def wait_loads(i):
        b, h = lax.div(i, heads), lax.rem(i, heads)
        settle(qg_buf.at[b, h], load_sem.at[0, b, h])
        settle(kv_buf.at[b, h], load_sem.at[1, b, h])

    def score_step(i, bufs):
        scores_buf, prob_grad_buf, peak_buf = bufs
        b, h = lax.div(i, heads), lax.rem(i, heads)
        keys = kv_buf[b, h, 0]
        values = kv_buf[b, h, 1]
        for n in range(blocks):
            span = pl.ds(n * query_block, query_block)
            scores = dot_nt(keys, qg_buf[b, h, 0, span, :])
            scores_buf[n] = scores
            peak_buf[n] = jnp.max(scores, axis=0, keepdims=True)
            prob_grad_buf[n] = dot_nt(values, qg_buf[b, h, 1, span, :])

    def grad_step(i, bufs):
        scores_buf, prob_grad_buf, peak_buf = bufs
        b, h = lax.div(i, heads), lax.rem(i, heads)
        key_grad = None
        for n in range(blocks):
            span = pl.ds(n * query_block, query_block)
            shifted = jnp.exp(scores_buf[n] - peak_buf[n])
            scale = 1.0 / jnp.sum(shifted, axis=0, keepdims=True)
            probs = shifted * scale
            probs_low = probs.astype(BF16)
            row_dot = jnp.sum(probs_low.astype(F32) * prob_grad_buf[n], axis=0, keepdims=True)
            score_low = (probs * (prob_grad_buf[n] - row_dot)).astype(BF16)
            value_term = dot_nn(probs_low, qg_buf[b, h, 1, span, :])
            key_term = dot_nn(score_low, qg_buf[b, h, 0, span, :])
            if key_grad is None:
                key_grad, value_grad = key_term, value_term
            else:
                key_grad, value_grad = key_grad + key_term, value_grad + value_term
        grads[:, pl.ds(pl.multiple_of(h * DK, DK), DK)] = key_grad.astype(BF16)
        grads[:, pl.ds(pl.multiple_of(inner + h * DK, DK), DK)] = value_grad.astype(BF16)

    even = (scores_even, prob_grad_even, peak_even)
    odd = (scores_odd, prob_grad_odd, peak_odd)

    def head_pair(i):
        wait_loads(i + 1)
        score_step(i + 1, odd)
        grad_step(i, even)
        following = jnp.minimum(i + 2, seqs * heads - 1)

        @pl.when(i + 2 < seqs * heads)
        def _():
            wait_loads(i + 2)

        score_step(following, even)
        grad_step(i + 1, odd)

    last = seqs - 1
    lower = z_me < chips // 2
    ahead = jnp.where(lower, chips - 1 - z_me, z_me)

    def order(j):
        rising = jnp.where(j < ahead, j, j - ahead)
        falling = chips - 1 - rising
        chip = jnp.where(lower == (j < ahead), falling, rising)
        return jnp.where(j == chips - 1, z_me, chip)

    def section_of(i):
        return lax.rem(s_me + i, sections)

    def piece(r):
        return pl.ds(r * piece_rows, piece_rows)

    def pair_copy(b, j):
        return pltpu.make_async_remote_copy(
            src_ref=part.at[b, j, CORES - 1 - c_me], dst_ref=pair_in.at[b, j],
            send_sem=pair_send, recv_sem=pair_recv.at[b, j],
            device_id={"tensor": partner}, device_id_type=MESH,
        )

    def section_copy(b, i, j, r):
        return pltpu.make_async_remote_copy(
            src_ref=part.at[b, j, c_me, section_of(i), piece(r)],
            dst_ref=section_in.at[b, i - 1, j, piece(r)],
            send_sem=section_send, recv_sem=section_recv.at[b, i - 1, j, r],
            device_id={"section": section_of(i)}, device_id_type=MESH,
        )

    def chain_copy(b, j, r):
        chip = order(j)
        right = chip > z_me
        target = jnp.where(right, z_me + 1, z_me - 1)
        slot = jnp.where(right | (chip != target), chip, chips)
        return pltpu.make_async_remote_copy(
            src_ref=line_out.at[b, j, piece(r)], dst_ref=line_in.at[b, slot, piece(r)],
            send_sem=line_send, recv_sem=line_recv.at[b, slot, r],
            device_id={"tensor": target * CORES + c_me}, device_id_type=MESH,
        )

    def chain_wait(b, slot, r):
        pltpu.make_async_remote_copy(
            src_ref=line_out.at[b, 0, piece(r)], dst_ref=line_in.at[b, slot, piece(r)],
            send_sem=line_send, recv_sem=line_recv.at[b, slot, r],
            device_id={"tensor": partner}, device_id_type=MESH,
        ).wait_recv()

    def share_copy(i):
        return pltpu.make_async_remote_copy(
            src_ref=scaled_hidden.at[z_me], dst_ref=scaled_hidden.at[z_me],
            send_sem=share_send, recv_sem=share_recv,
            device_id={"tensor": lax.rem(z_me + i, chips) * CORES + c_me}, device_id_type=MESH,
        )

    def stat_copies(src, dst, send, recv):
        return [
            pltpu.make_async_remote_copy(
                src_ref=src, dst_ref=dst.at[i - 1],
                send_sem=send, recv_sem=recv,
                device_id={"tensor": lax.rem(t_me + i, tensors)}, device_id_type=MESH,
            )
            for i in range(1, tensors)
        ]

    def square_copies():
        return stat_copies(square_out, square_in, square_send, square_recv)

    def cross_copies(b):
        return stat_copies(
            cross_out.at[b], cross_in.at[b], cross_send, cross_recv.at[b]
        )

    def lane_sums(x):
        total = dot_nt(jnp.ones((8, feats), F32), x, lax.Precision.HIGHEST)
        return total[0:1, :]

    def spread(row):
        return dot_tn(
            jnp.broadcast_to(row, (8, rows)), jnp.full((8, feats), 0.125, F32),
            lax.Precision.HIGHEST,
        )

    def loop(low, high, step):
        def run(i, carry):
            step(i)
            return carry

        lax.fori_loop(low, high, run, 0)

    def project(b, j):
        width = CORES * feats
        block = dot_nt(
            grads[...], w_buf[pl.ds(pl.multiple_of(order(j) * width, width), width), :]
        )
        for half in range(CORES):
            part[b, j, half] = block[:, half * feats : (half + 1) * feats].reshape(
                sections, rows, feats
            )
        pair_copy(b, j).start()

    def send_section(b, j):
        pair_copy(b, j).wait_recv()
        for i in range(1, sections):
            section = section_of(i)
            for r in range(pieces):
                part[b, j, c_me, section, piece(r)] += pair_in[b, j, section, piece(r)]
                section_copy(b, i, j, r).start()

    lead = 1 if chips > 1 else 0

    def project_all(b, between):
        def step(j):
            project(b, j)

            @pl.when(j == 1)
            def _():
                send_section(b, 0)

            @pl.when(j >= 3)
            def _():
                send_section(b, j - 2)

            between(j)

        loop(0, chips, step)

    def send_rest(b):
        loop(max(lead, chips - 2), chips, lambda j: send_section(b, j))

    def gather_piece(b, j, r, tally=False):
        total = part[b, j, c_me, s_me, piece(r)] + pair_in[b, j, s_me, piece(r)]
        for i in range(1, sections):
            section_copy(b, i, j, r).wait_recv()
            total = total + section_in[b, i - 1, j, piece(r)]
        line_out[b, j, piece(r)] = total
        chip = order(j)
        if tally:
            products[piece(r)] += scaled_hidden[chip, piece(r)] * total
        behind = jnp.where(chip > z_me, z_me > 0, z_me < chips - 1)

        @pl.when((j < chips - 1) & behind)
        def _():
            chain_wait(b, chip, r)
            line_out[b, j, piece(r)] += line_in[b, chip, piece(r)]

        @pl.when(j < chips - 1)
        def _():
            chain_copy(b, j, r).start()

    def finish_sum(b, finish):
        own = chips - 1
        for r in range(pieces):
            @pl.when(z_me > 0)
            def _():
                chain_wait(b, z_me, r)
                line_out[b, own, piece(r)] += line_in[b, z_me, piece(r)]

            @pl.when(z_me < chips - 1)
            def _():
                chain_wait(b, chips, r)
                line_out[b, own, piece(r)] += line_in[b, chips, piece(r)]

            finish(r)

    def send_cross(b, terms):
        cross_out[b] = lane_sums(terms)
        for copy in cross_copies(b):
            copy.start()

    def prepare_norm():
        settle(square_in, square_recv)
        for b in range(seqs):
            square = square_out[b]
            for i in range(tensors - 1):
                square = square + square_in[i, b]
            inverse = lax.rsqrt(square / model_width + EPSILON)
            inverse_gain[b] = gain[...] * spread(inverse)
            hidden_scaled[b] = hidden[b] * spread(inverse * inverse * inverse / model_width)

    def correction(b):
        cross = cross_out[b]
        settle(cross_in.at[b], cross_recv.at[b])
        for i in range(tensors - 1):
            cross = cross + cross_in[b, i]
        hidden_scaled[b] = hidden_scaled[b] * spread(cross)

    def write(b, r):
        total = line_out[b, chips - 1, piece(r)]
        out_ref[b, piece(r)] = total * inverse_gain[b, piece(r)] - hidden_scaled[b, piece(r)]

    steps = heads // 2
    total_pieces = chips * pieces

    def gather_span(b, low, high, tally=False):
        def step(n):
            gather_piece(b, lax.div(n, pieces), lax.rem(n, pieces), tally)

        loop(jnp.minimum(low, total_pieces), jnp.minimum(high, total_pieces), step)

    end_points = (0, 1, 2, 2, 3, 4, 6)
    mid_points = (2, 3, 5, 6, 6, 7)

    def reached(point):
        def count(starts):
            return sum(jnp.where(point >= start, 1, 0) for start in starts)

        return jnp.where(at_end, count(end_points), count(mid_points))

    def gather_until(b, point):
        gather_span(b, reached(point - 1), reached(point))

    points = steps + chips

    def sequence(b):
        def heads_step(j):
            head_pair(b * heads + 2 * j)

            @pl.when((b == 0) & (j == 0))
            def _():
                for copy in small_copies:
                    copy.wait()
                scaled_hidden[z_me] = gain[...] * hidden[last]
                pl.semaphore_wait(barrier, tensors - 1 + sections - 1)
                for i in range(1, chips):
                    share_copy(i).start()

            @pl.when(b > 0)
            def _():
                @pl.when(j == 0)
                def _():
                    send_rest(b - 1)

                gather_until(b - 1, j)

        def between(j):
            @pl.when(b > 0)
            def _():
                gather_until(b - 1, steps + j)

        loop(0, steps, heads_step)

        @pl.when(b == 0)
        def _():
            settle(w_buf, weight_sem)

        project_all(b, between)

    wait_loads(0)
    score_step(0, even)
    loop(0, seqs, sequence)
    send_rest(last)
    if seqs > 1:
        done = jnp.minimum(reached(points - 1), total_pieces)
        gather_span(last - 1, done, total_pieces)
    for b in range(seqs):
        square_out[b] = lane_sums(hidden[b] * hidden[b])
    for copy in square_copies():
        copy.start()
    products[...] = jnp.zeros_like(products)
    settle(scaled_hidden.at[pl.ds(0, chips - 1)], share_recv)
    gather_span(last, 0, total_pieces // 2, True)
    for b in range(last):
        finish_sum(b, lambda r: None)
        send_cross(b, line_out[b, chips - 1] * (gain[...] * hidden[b]))
    gather_span(last, total_pieces // 2, total_pieces, True)
    send_cross(last, products[...])
    prepare_norm()
    for b in range(last):
        correction(b)
        for r in range(pieces):
            write(b, r)
    correction(last)
    finish_sum(last, lambda r: write(last, r))

    settle(pair_in, pair_send)
    settle(section_in, section_send)
    settle(line_out.at[:, pl.ds(0, chips - 1)], line_send)
    settle(square_in, square_send)
    settle(cross_in, cross_send)
    settle(scaled_hidden.at[pl.ds(0, chips - 1)], share_send)


def per_device(
    sections, tensors,
    dec_queries, enc_keys, enc_values, out_grad, key_weight, value_weight, enc_hidden, enc_gain,
):
    _, seqs, dec_len, inner = dec_queries.shape
    enc_len = enc_keys.shape[2]
    heads = inner // DK
    model_width = key_weight.shape[1]
    chips = tensors // CORES
    feats = model_width // tensors
    rows = enc_len // sections
    dma = pltpu.SemaphoreType.DMA
    query_block = min(QUERY_BLOCK, dec_len)
    blocks = dec_len // query_block
    unit = [
        pltpu.VMEM((blocks, enc_len, query_block), F32),
        pltpu.VMEM((blocks, enc_len, query_block), F32),
        pltpu.VMEM((blocks, 1, query_block), F32),
    ]
    call = pl.pallas_call(
        functools.partial(body, sections, tensors, query_block),
        out_shape=jax.ShapeDtypeStruct((seqs, rows, feats), F32),
        in_specs=[pl.BlockSpec(memory_space=pl.ANY)] * 8,
        out_specs=pl.BlockSpec(memory_space=pltpu.VMEM),
        scratch_shapes=[
            pltpu.VMEM((seqs, heads, 2, dec_len, DK), BF16),
            pltpu.VMEM((seqs, heads, 2, enc_len, DK), BF16),
            pltpu.VMEM((model_width, 2 * inner), BF16),
            pltpu.VMEM((seqs, rows, feats), F32),
            pltpu.VMEM((1, feats), F32),
            pltpu.VMEM((enc_len, 2 * inner), BF16),
            *unit, *unit,
            pltpu.VMEM((seqs, chips, CORES, sections, rows, feats), F32),
            pltpu.VMEM((seqs, chips, sections, rows, feats), F32),
            pltpu.VMEM((seqs, sections - 1, chips, rows, feats), F32),
            pltpu.VMEM((seqs, chips, rows, feats), F32),
            pltpu.VMEM((seqs, chips + 1, rows, feats), F32),
            pltpu.VMEM((seqs, 1, rows), F32),
            pltpu.VMEM((tensors - 1, seqs, 1, rows), F32),
            pltpu.VMEM((seqs, 1, rows), F32),
            pltpu.VMEM((seqs, tensors - 1, 1, rows), F32),
            pltpu.VMEM((seqs, rows, feats), F32),
            pltpu.VMEM((seqs, rows, feats), F32),
            pltpu.VMEM((chips, rows, feats), F32),
            pltpu.VMEM((rows, feats), F32),
            dma((2, seqs, heads)),
            dma(()),
            dma((2,)),
            dma(()),
            dma((seqs, chips)),
            dma(()),
            dma((seqs, sections - 1, chips, PIECES)),
            dma(()),
            dma((seqs, chips + 1, PIECES)),
            dma(()),
            dma(()),
            dma(()),
            dma((seqs,)),
            dma(()),
            dma(()),
        ],
        compiler_params=pltpu.CompilerParams(
            collective_id=0, has_side_effects=True, vmem_limit_bytes=48 * 1024 * 1024
        ),
    )
    operands = (
        dec_queries, enc_keys, enc_values, out_grad, key_weight, value_weight,
        enc_hidden, enc_gain.reshape(1, feats),
    )
    return call(*(pltpu.with_memory_space_constraint(x, pltpu.HBM) for x in operands))


def solution(mesh):
    wide = P("section", "dp", None, "tensor")
    return jax.shard_map(
        functools.partial(per_device, mesh.shape["section"], mesh.shape["tensor"]),
        mesh=mesh,
        in_specs=(
            wide, wide, wide, wide,
            P("section", None, "tensor"),
            P("section", None, "tensor"),
            P("dp", "section", "tensor"),
            P("tensor"),
        ),
        out_specs=P("dp", "section", "tensor"),
        check_vma=False,
    )
```
